32 devices in a mesh: dp: 16 (over z, x, core), tensor: 2 (over y).
Axes of the slice: x: 2, y: 2, z: 4, core: 2. Of those that a mesh axis runs over, the one named last changes fastest.
Arguments:
- hidden_in: bfloat16 [2048, 16, 1024], P('tensor', 'dp'), may hold values from -6 to 6
- prefix_len: int32 [16], P('dp'), may hold values from 205 to 1024
- first_gain: bfloat16 [1024], P(('dp', 'tensor')), may hold values from 0.5 to 1.5
- query_heads: bfloat16 [1024, 96], P(('dp', 'tensor')), may hold values from -0.3125 to 0.3125
- query_basis: bfloat16 [1024, 384], P(('dp', 'tensor')), may hold values from -0.3125 to 0.3125
- key_heads: bfloat16 [1024, 32], P(('dp', 'tensor')), may hold values from -0.25 to 0.25
- key_basis: bfloat16 [1024, 128], P(('dp', 'tensor')), may hold values from -0.25 to 0.25
- value_heads: bfloat16 [1024, 32], P(('dp', 'tensor')), may hold values from -0.1875 to 0.1875
- value_basis: bfloat16 [1024, 128], P(('dp', 'tensor')), may hold values from -0.25 to 0.25
- output_weight: bfloat16 [1024, 1024], P('tensor', 'dp'), may hold values from -1 to 1
- second_gain: bfloat16 [1024], P(('dp', 'tensor')), may hold values from 0.5 to 1.5
- gate_weight: bfloat16 [1024, 2816], P('dp', 'tensor'), may hold values from -0.1875 to 0.1875
- up_weight: bfloat16 [1024, 2816], P('dp', 'tensor'), may hold values from -0.1875 to 0.1875
- down_weight: bfloat16 [2816, 1024], P('tensor', 'dp'), may hold values from -0.15625 to 0.15625
- grad_out: bfloat16 [2048, 16, 1024], P('tensor', 'dp'), may hold values from -6 to 6
Outputs:
- hidden_out: bfloat16 [2048, 16, 1024], P('tensor', 'dp')
- grad_in: float32 [2048, 16, 1024], P('tensor', 'dp')
- first_gain_grad: float32 [1024], P(('dp', 'tensor'))
- query_heads_grad: float32 [1024, 96], P(('dp', 'tensor'))
- query_basis_grad: float32 [1024, 384], P(('dp', 'tensor'))
- key_heads_grad: float32 [1024, 32], P(('dp', 'tensor'))
- key_basis_grad: float32 [1024, 128], P(('dp', 'tensor'))
- value_heads_grad: float32 [1024, 32], P(('dp', 'tensor'))
- value_basis_grad: float32 [1024, 128], P(('dp', 'tensor'))
- output_weight_grad: float32 [1024, 1024], P('tensor', 'dp')
- second_gain_grad: float32 [1024], P(('dp', 'tensor'))
- gate_weight_grad: float32 [1024, 2816], P('dp', 'tensor')
- up_weight_grad: float32 [1024, 2816], P('dp', 'tensor')
- down_weight_grad: float32 [2816, 1024], P('tensor', 'dp')
The draws below stay inside these ranges and needn't reach their ends.
All inputs are finite; a program needn't handle non-finite values.
Results may differ from the reference program's by a relative error of at most 0.023.
The reference program's roundings to bfloat16 on the way count: a program that leaves them out, or rounds other values in their place, can miss the bound.
Values may be sent and summed in bfloat16 or wider, within the bound.
A program may use at most 320 MiB of HBM per device.

```python
import math
import jax
import jax.numpy as jnp
from jax import lax

D = 1024
HEADS = 16
DH = 64
RQ = 6
RKV = 2
FF = 2816
LEN = 2048
QB = 512
SEQS = 16


def place_ends(result, rng, low, largest):
    shape = result.shape
    place = [jax.random.randint(jax.random.fold_in(rng, axis), (), 0, shape[axis]) for axis in range(len(shape))]
    result = result.at[tuple(place)].set(low)
    longest = shape.index(max(shape))
    place[longest] = (place[longest] + 1) % shape[longest]
    return result.at[tuple(place)].set(largest)


def steps_of(own_key, shape, split, smallest, largest):
    def one(dim, parts):
        heights = jax.random.uniform(jax.random.fold_in(jax.random.fold_in(own_key, 6), dim), (parts,), jnp.float32, smallest / len(split), largest / len(split))
        return jnp.repeat(jnp.exp(heights), shape[dim] // parts).reshape((-1,) + (1,) * (len(shape) - dim - 1))

    gain = one(*split[0])
    for cut in split[1:]:
        gain = gain * one(*cut)
    return gain


def normal_values(key, extent, width, limit, shards=(), kind=jnp.bfloat16):
    values = width * jax.random.normal(key, extent, jnp.float32)
    if shards:
        values = values * steps_of(key, extent, shards, -0.22, 0.18)
    return jnp.clip(values, -limit, limit).astype(kind)


def setup_inputs(seed: int = 0) -> dict:
    arg_keys = jax.random.split(jax.random.key(seed), 16)
    hidden_in = normal_values(arg_keys[0], (LEN, SEQS, D), 1.0, 6.0, ((0, 2), (1, 16)))
    prefix_len = place_ends(jax.random.randint(arg_keys[1], (SEQS,), LEN // 10 + 1, LEN // 2 + 1), jax.random.fold_in(arg_keys[1], 1), LEN // 10 + 1, (LEN // 2 + 1) - 1).astype(jnp.int32)
    first_gain = jnp.clip(1.0 + 0.1 * jax.random.normal(arg_keys[2], (D,), jnp.float32), 0.5, 1.5).astype(jnp.bfloat16)
    query_heads = normal_values(arg_keys[3], (D, HEADS * RQ), (D // 3) ** -0.5, 0.3125, ((0, 32),))
    query_basis = normal_values(arg_keys[4], (D, RQ * DH), (D // 3) ** -0.5, 0.3125, ((0, 32),))
    key_heads = normal_values(arg_keys[5], (D, HEADS * RKV), (D // 2) ** -0.5, 0.25, ((0, 32),))
    key_basis = normal_values(arg_keys[6], (D, RKV * DH), (D // 2) ** -0.5, 0.25, ((0, 32),))
    value_heads = normal_values(arg_keys[7], (D, HEADS * RKV), D ** -0.5, 0.1875, ((0, 32),))
    value_basis = normal_values(arg_keys[8], (D, RKV * DH), (D // 2) ** -0.5, 0.25, ((0, 32),))
    output_weight = normal_values(arg_keys[9], (HEADS * DH, D), (HEADS * DH // 32) ** -0.5, 1.0, ((0, 2), (1, 16)))
    second_gain = jnp.clip(1.0 + 0.1 * jax.random.normal(arg_keys[10], (D,), jnp.float32), 0.5, 1.5).astype(jnp.bfloat16)
    gate_weight = normal_values(arg_keys[11], (D, FF), D ** -0.5, 0.1875, ((0, 16), (1, 2)))
    up_weight = normal_values(arg_keys[12], (D, FF), D ** -0.5, 0.1875, ((0, 16), (1, 2)))
    down_weight = normal_values(arg_keys[13], (FF, D), (FF // 2) ** -0.5, 0.15625, ((0, 2), (1, 16)))
    grad_out = normal_values(arg_keys[14], (LEN, SEQS, D), 1.0, 6.0, ((0, 2), (1, 16)))
    return {"hidden_in": hidden_in, "prefix_len": prefix_len, "first_gain": first_gain, "query_heads": query_heads, "query_basis": query_basis, "key_heads": key_heads, "key_basis": key_basis, "value_heads": value_heads, "value_basis": value_basis, "output_weight": output_weight, "second_gain": second_gain, "gate_weight": gate_weight, "up_weight": up_weight, "down_weight": down_weight, "grad_out": grad_out}


EPS = 1e-05
ROPE_BASE = 10000.0
NEG_FILL = -1e+30

@jax.custom_vjp
def low(v):
    return lax.optimization_barrier(v.astype(jnp.bfloat16)).astype(jnp.float32)

@jax.custom_vjp
def low_back(v):
    return v

def low_keep(v):
    return (low(v), None)

def low_pass(kept, grad):
    return (grad,)

def back_keep(v):
    return (v, None)

def back_low(kept, grad):
    return (low(grad),)
low.defvjp(low_keep, low_pass)
low_back.defvjp(back_keep, back_low)

def rotate(basis, offset, turn_sign):
    half_dim = basis.shape[-1] // 2
    length = basis.shape[0]
    frequency = jnp.exp(jnp.arange(half_dim, dtype=jnp.float32) * (-math.log(ROPE_BASE) / half_dim))
    positions = (offset + jnp.arange(length, dtype=jnp.int32)).astype(jnp.float32)
    angles = positions[:, None] * frequency[None, :]
    view_shape = (length,) + (1,) * (basis.ndim - 2) + (half_dim,)
    cosine = jnp.cos(angles).reshape(view_shape)
    sine_part = (turn_sign * jnp.sin(angles)).reshape(view_shape)
    lower_half = basis[..., :half_dim]
    upper_half = basis[..., half_dim:]
    return jnp.concatenate([lower_half * cosine - upper_half * sine_part, upper_half * cosine + lower_half * sine_part], axis=-1)

def normalize(values, gain_row):
    return values * lax.rsqrt(lax.optimization_barrier(jnp.mean(values * values, axis=-1, keepdims=True)) + EPS) * gain_row

def product(left, right):
    return jnp.dot(left, right, preferred_element_type=jnp.float32, precision=lax.Precision.HIGHEST)

def layer(hidden, prefix, first_gain, query_heads, query_basis, key_heads, key_basis, value_heads, value_basis, output_weight, second_gain, gate_weight, up_weight, down_weight):
    length = hidden.shape[0]
    highest = lax.Precision.HIGHEST
    normed = low(normalize(hidden, first_gain))

    def factor(weight):
        return low(low_back(product(normed, weight)))
    query_mix = factor(query_heads).reshape(length, HEADS, RQ)
    query_base = rotate(factor(query_basis).reshape(length, RQ, DH), 0, 1.0)
    key_mix = factor(key_heads).reshape(length, HEADS, RKV)
    key_base = rotate(factor(key_basis).reshape(length, RKV, DH), 0, 1.0)
    value_mix = factor(value_heads).reshape(length, HEADS, RKV)
    value_base = factor(value_basis).reshape(length, RKV, DH)
    queries = low(low_back(jnp.einsum('lhr,lrd->lhd', query_mix, query_base, precision=highest) / RQ))
    key_rows = low(low_back(jnp.einsum('lhr,lrd->lhd', key_mix, key_base, precision=highest) / RKV))
    value_rows = low(low_back(jnp.einsum('lhr,lrd->lhd', value_mix, value_base, precision=highest) / RKV))
    positions = jnp.arange(length, dtype=jnp.int32)
    score_scale = 1.0 / math.sqrt(DH)

    def attend_block(row_start):
        query_block = lax.dynamic_slice_in_dim(queries, row_start, QB, 0)
        raw = jnp.einsum('qhd,khd->hqk', query_block, key_rows, precision=highest) * score_scale
        scores = low_back(raw)
        rows = row_start + jnp.arange(QB, dtype=jnp.int32)
        visible = (positions[None, :] <= rows[:, None]) | (positions[None, :] < prefix)
        scores = jnp.where(visible[None], scores, NEG_FILL)
        row_max = lax.optimization_barrier(jnp.max(scores, axis=-1, keepdims=True))
        shifted = jnp.exp(scores - row_max)
        attn_probs = shifted / lax.optimization_barrier(jnp.sum(shifted, axis=-1, keepdims=True))
        return jnp.einsum('hqk,khd->qhd', low(attn_probs), value_rows, precision=highest)
    block_starts = jnp.arange(0, length, QB, dtype=jnp.int32)
    attended = lax.map(jax.checkpoint(attend_block), block_starts).reshape(length, HEADS * DH)
    attended = low(low_back(attended))
    middle = hidden + low_back(product(attended, output_weight))
    normed_second = low(normalize(middle, second_gain))
    gate_preactivation = low_back(product(normed_second, gate_weight))
    up_projection_rows = low_back(product(normed_second, up_weight))
    swish_output = low(gate_preactivation * jax.nn.sigmoid(gate_preactivation) * up_projection_rows)
    return middle + low_back(product(swish_output, down_weight))

def reference(hidden_in, prefix_len, first_gain, query_heads, query_basis, key_heads, key_basis, value_heads, value_basis, output_weight, second_gain, gate_weight, up_weight, down_weight, grad_out):
    params = tuple((weight.astype(jnp.float32) for weight in (first_gain, query_heads, query_basis, key_heads, key_basis, value_heads, value_basis, output_weight, second_gain, gate_weight, up_weight, down_weight)))
    inputs = jnp.moveaxis(hidden_in.astype(jnp.float32), 1, 0)
    cotangents = jnp.moveaxis(grad_out.astype(jnp.float32), 1, 0)

    def one_sequence(totals, seq_item):
        hidden, prefix, cotangent = seq_item

        def forward(hidden_rows, *weights):
            return layer(hidden_rows, prefix, *weights)
        output, pullback = jax.vjp(forward, hidden, *params)
        grads = pullback(cotangent)
        new_totals = tuple((total + grad for total, grad in zip(totals, grads[1:])))
        return (new_totals, (output.astype(jnp.bfloat16), grads[0]))
    zero_init = tuple((jnp.zeros(weight.shape, jnp.float32) for weight in params))
    totals, (outputs, input_grads) = lax.scan(one_sequence, zero_init, (inputs, prefix_len, cotangents))
    hidden_out = jnp.moveaxis(outputs, 0, 1)
    grad_in = jnp.moveaxis(input_grads, 0, 1)
    return (hidden_out, grad_in, totals[0], totals[1], totals[2], totals[3], totals[4], totals[5], totals[6], totals[7], totals[8], totals[9], totals[10], totals[11])
```

```python
import functools
import math

import jax
import jax.numpy as jnp
from jax import lax
from jax.experimental import pallas as pl
from jax.experimental.pallas import tpu as pltpu
from jax.sharding import PartitionSpec as P

HEADS = 16
DH = 64
RQ = 6
RKV = 2
EPS = 1e-05
ROPE_BASE = 10000.0
NEG_FILL = -1e30
QB = 256
KC = 512
RB = 256
BF = jnp.bfloat16
F32 = jnp.float32

KV_COLS = 384
Q_COLS = 512
PACK = KV_COLS + Q_COLS
Q_BASIS = RQ * DH
Q_HEADS = HEADS * RQ
KV_HEADS = HEADS * RKV

NN = (((1,), (0,)), ((), ()))
NT = (((1,), (1,)), ((), ()))
TN = (((0,), (0,)), ((), ()))


def dot(left, right, dims=NN):
    return lax.dot_general(left, right, dims, preferred_element_type=F32)


def swap(value, axis, mask):
    count = lax.axis_size(axis)
    return lax.ppermute(value, axis, [(i, i ^ mask) for i in range(count)])


def stage_masks(stage):
    if stage == "y":
        return "tensor", list(range(1, lax.axis_size("tensor")))
    if stage == "z":
        return "dp", [4 * i for i in range(1, lax.axis_size("dp") // 4)]
    return "dp", [2 if stage == "x" else 1]


def gather_stage(value, stage):
    axis, masks = stage_masks(stage)
    return jnp.stack([value] + [swap(value, axis, mask) for mask in masks])


def stage_index(stage):
    if stage == "y":
        return lax.axis_index("tensor")
    place = lax.axis_index("dp")
    if stage == "z":
        return place // 4
    if stage == "x":
        return (place // 2) % 2
    return place % 2


def scatter_stage(pick, stage):
    axis, masks = stage_masks(stage)
    mine = stage_index(stage)
    got = []
    for step, mask in enumerate(masks, 1):
        got.append(swap(pick(jnp.bitwise_xor(mine, step)), axis, mask))
    return got


def lanes(rows):
    return lax.broadcasted_iota(jnp.int32, (rows, 128), 1)


def turned(x, cosine, sine, sign):
    lane = lanes(x.shape[0])
    low = (lane % DH) < (DH // 2)
    up = pltpu.roll(x, 128 - DH // 2, 1)
    down = pltpu.roll(x, DH // 2, 1)
    return x * cosine + jnp.where(low, -sign * up, sign * down) * sine


def both_halves(pair, odd):
    lane = lanes(pair.shape[0])
    other = pltpu.roll(pair, DH, 1)
    one = jnp.where((lane < DH) != bool(odd), pair, other)
    return one


def doubled(tile):
    return jnp.concatenate([tile, tile], axis=1)


def mix_rows(tiles, mixes, spread_ref, rank, out_ref):
    width = out_ref.shape[1]
    for block in range(width // 256):
        total = None
        for r in range(rank):
            at = r * width + block * 256
            term = dot(mixes, spread_ref[:, at : at + 256]) * doubled(tiles[r])
            total = term if total is None else total + term
        out_ref[:, block * 256 : (block + 1) * 256] = (total * (1.0 / rank)).astype(BF)


def unmix_rows(tiles, mixes, spread_ref, rank, grad_ref):
    width = grad_ref.shape[1]
    mix_grad = None
    base_grads = [None] * rank
    for block in range(width // 256):
        grad = grad_ref[:, block * 256 : (block + 1) * 256].astype(F32)
        for r in range(rank):
            at = r * width + block * 256
            spread = spread_ref[:, at : at + 256]
            term = dot((grad * doubled(tiles[r])).astype(BF), spread, NT)
            mix_grad = term if mix_grad is None else mix_grad + term
            part = dot(mixes, spread) * grad
            part = part[:, :128] + part[:, 128:]
            base_grads[r] = part if base_grads[r] is None else base_grads[r] + part
    scale = 1.0 / rank
    base_grads = [(part + pltpu.roll(part, DH, 1)) * scale for part in base_grads]
    return mix_grad * scale, base_grads


def query_tiles(factor_ref, cosine, sine):
    tiles = []
    for pair in range(RQ // 2):
        base = turned(factor_ref[:, pair * 128 : (pair + 1) * 128].astype(F32), cosine, sine, 1.0)
        tiles += [both_halves(base, 0), both_halves(base, 1)]
    return tiles


def key_tiles(factor_ref, cosine, sine):
    base = turned(factor_ref[:, :128].astype(F32), cosine, sine, 1.0)
    return [both_halves(base, 0), both_halves(base, 1)]


def value_tiles(factor_ref):
    base = factor_ref[:, 128:256].astype(F32)
    return [both_halves(base, 0), both_halves(base, 1)]


def query_kernel(factor_ref, cos_ref, sin_ref, spread_ref, out_ref):
    tiles = query_tiles(factor_ref, cos_ref[...], sin_ref[...])
    mix_rows(tiles, factor_ref[:, Q_BASIS:Q_COLS], spread_ref, RQ, out_ref)


def key_value_kernel(me_ref, factor_ref, cos_ref, sin_ref, kspread_ref, vspread_ref, k_ref, v_ref):
    mixes = factor_ref[0, :, 256:KV_COLS]
    factor = factor_ref.at[0]
    mix_rows(key_tiles(factor, cos_ref[...], sin_ref[...]), mixes, kspread_ref, RKV, k_ref)
    mix_rows(value_tiles(factor), mixes, vspread_ref, RKV, v_ref)


def query_back_kernel(factor_ref, cos_ref, sin_ref, spread_ref, grad_ref, out_ref):
    cosine, sine = cos_ref[...], sin_ref[...]
    tiles = query_tiles(factor_ref, cosine, sine)
    mix_grad, bases = unmix_rows(tiles, factor_ref[:, Q_BASIS:Q_COLS], spread_ref, RQ, grad_ref)
    lane = lanes(RB)
    for pair in range(RQ // 2):
        base = jnp.where(lane < DH, bases[2 * pair], bases[2 * pair + 1])
        out_ref[:, pair * 128 : (pair + 1) * 128] = turned(base, cosine, sine, -1.0).astype(BF)
    out_ref[:, Q_BASIS:] = mix_grad.astype(BF)


def key_value_back_kernel(
    me_ref, factor_ref, cos_ref, sin_ref, kspread_ref, vspread_ref, kgrad_ref, vgrad_ref, out_ref
):
    cosine, sine = cos_ref[...], sin_ref[...]
    factor = factor_ref.at[0]
    mixes = factor_ref[0, :, 256:KV_COLS]
    lane = lanes(RB)
    kmix, kbase = unmix_rows(key_tiles(factor, cosine, sine), mixes, kspread_ref, RKV, kgrad_ref)
    vmix, vbase = unmix_rows(value_tiles(factor), mixes, vspread_ref, RKV, vgrad_ref)
    keys = turned(jnp.where(lane < DH, kbase[0], kbase[1]), cosine, sine, -1.0)
    out_ref[0, :, :128] = keys.astype(BF)
    out_ref[0, :, 128:256] = jnp.where(lane < DH, vbase[0], vbase[1]).astype(BF)
    out_ref[0, :, 256:] = (kmix + vmix).astype(BF)


def spread_matrix(rank, first):
    width = HEADS * DH
    row = lax.broadcasted_iota(jnp.int32, (128, rank * width), 0)
    col = lax.broadcasted_iota(jnp.int32, (128, rank * width), 1)
    return (row == first + ((col % width) // DH) * rank + col // width).astype(BF)


def whole_block(shape):
    return pl.BlockSpec(shape, lambda i, *_: (0,) * len(shape))


def row_block(cols):
    return pl.BlockSpec((RB, cols), lambda i, *_: (i, 0))


PARAMS = pltpu.CompilerParams(vmem_limit_bytes=60 << 20)


def build_queries(factors, cosine, sine, spread):
    rows, width = factors.shape[0], HEADS * DH
    return pl.pallas_call(
        query_kernel,
        out_shape=jax.ShapeDtypeStruct((rows, width), BF),
        grid=(rows // RB,),
        in_specs=[row_block(Q_COLS), row_block(128), row_block(128), whole_block(spread.shape)],
        out_specs=row_block(width),
        compiler_params=PARAMS,
        name="build_queries",
    )(factors, cosine, sine, spread)


def relative_rows(parts, cols):
    blocks = parts // RB

    def place(i, me):
        return (jnp.bitwise_xor(i // blocks, me[0]), i % blocks, 0)

    return pl.BlockSpec((1, RB, cols), place)


def build_keys(me, factors, cosine, sine, kspread, vspread):
    rows, width = factors.shape[0] * factors.shape[1], HEADS * DH
    return pl.pallas_call(
        key_value_kernel,
        out_shape=(jax.ShapeDtypeStruct((rows, width), BF),) * 2,
        grid_spec=pltpu.PrefetchScalarGridSpec(
            num_scalar_prefetch=1,
            grid=(rows // RB,),
            in_specs=[
                relative_rows(factors.shape[1], KV_COLS),
                row_block(128),
                row_block(128),
                whole_block(kspread.shape),
                whole_block(vspread.shape),
            ],
            out_specs=(row_block(width), row_block(width)),
        ),
        compiler_params=PARAMS,
        name="build_keys",
    )(me, factors, cosine, sine, kspread, vspread)


def queries_back(factors, cosine, sine, spread, grad):
    rows = factors.shape[0]
    return pl.pallas_call(
        query_back_kernel,
        out_shape=jax.ShapeDtypeStruct((rows, Q_COLS), BF),
        grid=(rows // RB,),
        in_specs=[
            row_block(Q_COLS),
            row_block(128),
            row_block(128),
            whole_block(spread.shape),
            row_block(HEADS * DH),
        ],
        out_specs=row_block(Q_COLS),
        compiler_params=PARAMS,
        name="queries_back",
    )(factors, cosine, sine, spread, grad)


def keys_back(me, factors, cosine, sine, kspread, vspread, kgrad, vgrad):
    rows = kgrad.shape[0]
    return pl.pallas_call(
        key_value_back_kernel,
        out_shape=jax.ShapeDtypeStruct(factors.shape, BF),
        grid_spec=pltpu.PrefetchScalarGridSpec(
            num_scalar_prefetch=1,
            grid=(rows // RB,),
            in_specs=[
                relative_rows(factors.shape[1], KV_COLS),
                row_block(128),
                row_block(128),
                whole_block(kspread.shape),
                whole_block(vspread.shape),
                row_block(HEADS * DH),
                row_block(HEADS * DH),
            ],
            out_specs=relative_rows(factors.shape[1], KV_COLS),
        ),
        compiler_params=PARAMS,
        name="keys_back",
    )(me, factors, cosine, sine, kspread, vspread, kgrad, vgrad)


def forward_kernel(where_ref, q_ref, k_ref, v_ref, o_ref, lse_ref):
    start, prefix = where_ref[0], where_ref[1]
    rows, keys = q_ref.shape[0], k_ref.shape[0]
    lane = lanes(QB)
    for block in range(rows // QB):
        at = slice(block * QB, (block + 1) * QB)
        width = keys - rows + (block + 1) * QB
        query = q_ref[at, :] * BF(0.125)
        row = start + block * QB + lax.broadcasted_iota(jnp.int32, (QB, 1), 0)
        bound = jnp.maximum(row + 1, prefix)
        col = lax.broadcasted_iota(jnp.int32, (QB, width), 1)
        key, value = k_ref[:width, :], v_ref[:width, :]
        results = []
        for half in range(2):
            one = jnp.where((lane < DH) != bool(half), query, BF(0))
            scores = jnp.where(col < bound, dot(one, key, NT), NEG_FILL)
            top = jnp.max(scores, axis=-1, keepdims=True)
            shifted = jnp.exp(scores - top)
            total = jnp.sum(shifted, axis=-1, keepdims=True)
            results.append(dot(shifted.astype(BF), value) / total)
            log_total = jnp.broadcast_to(top + jnp.log(total), (QB, 128))
            lse_ref[0, half : half + 1, at] = log_total.T[0:1, :]
        o_ref[at, :] = jnp.where(lane < DH, results[0], results[1]).astype(BF)


def backward_kernel(
    where_ref, q_ref, k_ref, v_ref, g_ref, o_ref, lse_ref, dq_ref, dk_ref, dv_ref, dk_sum, dv_sum
):
    start, prefix = where_ref[0], where_ref[1]
    rows, keys = q_ref.shape[0], k_ref.shape[0]
    lane = lanes(QB)
    dk_sum[...] = jnp.zeros_like(dk_sum)
    dv_sum[...] = jnp.zeros_like(dv_sum)
    for block in range(rows // QB):
        at = slice(block * QB, (block + 1) * QB)
        width = keys - rows + (block + 1) * QB
        query = q_ref[at, :] * BF(0.125)
        grad = g_ref[at, :]
        product = (grad.astype(F32) * o_ref[at, :].astype(F32)).T
        inner = [
            jnp.sum(product[:DH], axis=0, keepdims=True),
            jnp.sum(product[DH:], axis=0, keepdims=True),
        ]
        col = start + block * QB + lax.broadcasted_iota(jnp.int32, (1, QB), 1)
        bound = jnp.maximum(col + 1, prefix)
        query_of = [jnp.where((lane < DH) != bool(h), query, BF(0)) for h in range(2)]
        grad_of = [jnp.where((lane < DH) != bool(h), grad, BF(0)) for h in range(2)]
        log_of = [lse_ref[0, h : h + 1, at] for h in range(2)]
        query_both = jnp.concatenate(query_of, axis=0)
        grad_both = jnp.concatenate(grad_of, axis=0)
        sums = [jnp.zeros((QB, 128), F32)] * 2
        done = 0
        while done < width:
            size = min(KC, width - done)
            key, value = k_ref[done : done + size, :], v_ref[done : done + size, :]
            row = done + lax.broadcasted_iota(jnp.int32, (size, QB), 0)
            visible = row < bound
            probs, grads = [], []
            for h in range(2):
                scores = dot(key, query_of[h], NT)
                prob = jnp.where(visible, jnp.exp(scores - log_of[h]), 0.0)
                part = dot(value, grad_of[h], NT)
                grad_score = (prob * (part - inner[h])).astype(BF)
                probs.append(prob.astype(BF))
                grads.append(grad_score)
                sums[h] = sums[h] + dot(grad_score, key, TN)
            dk_sum[done : done + size, :] += dot(jnp.concatenate(grads, axis=1), query_both)
            dv_sum[done : done + size, :] += dot(jnp.concatenate(probs, axis=1), grad_both)
            done += size
        dq_ref[at, :] = (jnp.where(lane < DH, sums[0], sums[1]) * 0.125).astype(BF)
    dk_ref[...] = dk_sum[...].astype(BF)
    dv_ref[...] = dv_sum[...].astype(BF)


def attention(where, query, key, value):
    rows, keys, pairs = query.shape[0], key.shape[0], query.shape[1] // 128
    local = pl.BlockSpec((rows, 128), lambda h: (0, h))
    whole = pl.BlockSpec((keys, 128), lambda h: (0, h))
    work = pairs * 2 * rows * keys
    return pl.pallas_call(
        forward_kernel,
        out_shape=(
            jax.ShapeDtypeStruct(query.shape, BF),
            jax.ShapeDtypeStruct((pairs, 8, rows), F32),
        ),
        grid=(pairs,),
        in_specs=[pl.BlockSpec(memory_space=pltpu.SMEM), local, whole, whole],
        out_specs=(local, pl.BlockSpec((1, 8, rows), lambda h: (h, 0, 0))),
        compiler_params=PARAMS,
        cost_estimate=pl.CostEstimate(
            flops=work * 4 * 256, transcendentals=work, bytes_accessed=2 * 2 * (query.size + key.size)
        ),
        name="attention",
    )(where, query, key, value)


def attention_back(where, query, key, value, grad, out, log_total, first, count):
    rows, keys = query.shape[0], key.shape[0]
    local = pl.BlockSpec((rows, 128), lambda h: (0, first + h))
    whole = pl.BlockSpec((keys, 128), lambda h: (0, first + h))
    local_out = pl.BlockSpec((rows, 128), lambda h: (0, h))
    whole_out = pl.BlockSpec((keys, 128), lambda h: (0, h))
    work = count * 2 * rows * keys
    return pl.pallas_call(
        backward_kernel,
        out_shape=(
            jax.ShapeDtypeStruct((rows, 128 * count), BF),
            jax.ShapeDtypeStruct((keys, 128 * count), BF),
            jax.ShapeDtypeStruct((keys, 128 * count), BF),
        ),
        grid=(count,),
        in_specs=[
            pl.BlockSpec(memory_space=pltpu.SMEM),
            local,
            whole,
            whole,
            local,
            local,
            pl.BlockSpec((1, 8, rows), lambda h: (first + h, 0, 0)),
        ],
        out_specs=(local_out, whole_out, whole_out),
        scratch_shapes=[pltpu.VMEM((keys, 128), F32)] * 2,
        compiler_params=PARAMS,
        cost_estimate=pl.CostEstimate(
            flops=work * 10 * 256,
            transcendentals=work,
            bytes_accessed=2 * count * 128 * (4 * rows + 4 * keys),
        ),
        name="attention_back",
    )(where, query, key, value, grad, out, log_total)


def rel_split(index, sizes):
    parts = []
    for size in reversed(sizes):
        parts.append(index % size)
        index = index // size
    return parts[::-1]


def place_small(me, own, got, nd, nt):
    half, rows, cols = own.shape

    def kernel(me_ref, own_ref, got_ref, out_ref):
        for core in range(2):
            source = own_ref if core == 0 else got_ref
            for i in range(half):
                y, x, z = rel_split(i, (nt, 2, nd // 4))
                offset = (z * 4 + x * 2 + core) * nt + y
                out_ref[jnp.bitwise_xor(me_ref[0], offset)] = source[i]

    vmem = pl.BlockSpec(memory_space=pltpu.VMEM)
    return pl.pallas_call(
        kernel,
        out_shape=jax.ShapeDtypeStruct((2 * half, rows, cols), BF),
        in_specs=[pl.BlockSpec(memory_space=pltpu.SMEM), vmem, vmem],
        out_specs=vmem,
        compiler_params=PARAMS,
        name="place_small",
    )(me, own, got)


def place_weights(me, first, second, widths, nd, nt):
    half, rows = first[0].shape[:2]
    nz = nd // 4

    def spot(i):
        core, y, x, z = rel_split(i, (2, nt, 2, nz))
        return core, y, x, z

    def in_first(core_wanted):
        def index(i, me):
            low = i if core_wanted == 0 else i - half
            return (jnp.clip(low, 0, half - 1), 0, 0)

        return index

    def in_second(core_wanted):
        def index(i, me):
            low = jnp.clip(i if core_wanted == 0 else i - half, 0, half - 1)
            y, x, z = rel_split(low, (nt, 2, nz))
            return ((x * nt + y) * nz + z, 0, 0)

        return index

    aligned = all(width % 128 == 0 for width in widths)

    def out_index(i, me):
        core, y, x, z = spot(i)
        row = jnp.bitwise_xor(me[0], z * 4 + x * 2 + core)
        share = jnp.bitwise_xor(me[1], y)
        return (row, share) if aligned else (share, row, 0)

    def out_block(width):
        return pl.BlockSpec((rows, width) if aligned else (None, rows, width), out_index)

    def out_type(width):
        shape = (nd * rows, nt * width) if aligned else (nt, nd * rows, width)
        return jax.ShapeDtypeStruct(shape, BF)

    def kernel(me_ref, a_own, a_got, b_own, b_got, *outs):
        def move(a, b):
            at = 0
            for out, width in zip(outs[:2], widths[:2]):
                out[...] = a[0, :, at : at + width]
                at += width
            at = 0
            for out, width in zip(outs[2:], widths[2:]):
                out[...] = b[0, :, at : at + width]
                at += width

        @pl.when(pl.program_id(0) < half)
        def _():
            move(a_own, b_own)

        @pl.when(pl.program_id(0) >= half)
        def _():
            move(a_got, b_got)

    placed = pl.pallas_call(
        kernel,
        out_shape=tuple(out_type(width) for width in widths),
        grid_spec=pltpu.PrefetchScalarGridSpec(
            num_scalar_prefetch=1,
            grid=(2 * half,),
            in_specs=[
                pl.BlockSpec((1, rows, first[0].shape[2]), in_first(0)),
                pl.BlockSpec((1, rows, first[0].shape[2]), in_first(1)),
                pl.BlockSpec((1, rows, second[0].shape[2]), in_second(0)),
                pl.BlockSpec((1, rows, second[0].shape[2]), in_second(1)),
            ],
            out_specs=tuple(out_block(width) for width in widths),
        ),
        compiler_params=PARAMS,
        name="place_weights",
    )(me, *first, *second)
    if aligned:
        return placed
    return [jnp.moveaxis(array, 0, 1).reshape(nd * rows, -1) for array in placed]


def gather_dense(packed, order):
    held = packed
    for stage in order:
        held = gather_stage(held, stage)
        held = held.reshape((-1,) + packed.shape)
    return held, swap(held, "dp", 1)


def pick_of(parts, index, count):
    if count == 2:
        return jnp.where(index == 0, parts[0], parts[1])
    return lax.dynamic_index_in_dim(jnp.stack(parts), index, 0, keepdims=False)


def scatter_sum(parts, order):
    nt, nd = len(parts), lax.axis_size("dp")
    widths = [array.shape[1] for array in parts[0]]
    rows = parts[0][0].shape[0] // nd
    nz = nd // 4
    held = [[array.reshape(nz, 2, 2, rows, -1) for array in share] for share in parts]
    lead = ["z", "x", "core"]

    def take(array, stage, index):
        return lax.dynamic_index_in_dim(array, index, lead.index(stage), keepdims=False)

    for number, stage in enumerate(order):
        last = number == len(order) - 1
        mine = stage_index(stage)
        if stage == "y":

            def pick(index):
                return [pick_of([held[t][a] for t in range(nt)], index, nt) for a in range(len(widths))]

            def packed(index):
                return jnp.concatenate(pick(index), axis=-1)

            got = scatter_stage(packed, stage)
            kept = [pick(mine)]
        else:

            def packed(index):
                return jnp.concatenate(
                    [take(array, stage, index) for share in held for array in share], axis=-1
                )

            got = scatter_stage(packed, stage)
            kept = [[take(array, stage, mine) for array in share] for share in held]
            lead.remove(stage)
        at = 0
        result = []
        for share in kept:
            row = []
            for array in share:
                width = array.shape[-1]
                total = array.astype(F32)
                for piece in got:
                    total = total + piece[..., at : at + width].astype(F32)
                at += width
                row.append(total if last else total.astype(BF))
            result.append(row)
        held = result
    return held[0]


def rms_scale(values):
    return lax.rsqrt(jnp.mean(values * values, axis=-1, keepdims=True) + EPS)


def norm_back(values, row_scale, gain_row, upstream):
    weighted = upstream * gain_row
    inner_term = jnp.mean(values * weighted, axis=-1, keepdims=True)
    grad_values = row_scale * weighted - values * (row_scale * row_scale * row_scale) * inner_term
    gain_term = jnp.sum(upstream * values * row_scale, axis=0)
    return grad_values, gain_term


def per_device(
    hidden_in,
    prefix_len,
    first_gain,
    query_heads,
    query_basis,
    key_heads,
    key_basis,
    value_heads,
    value_basis,
    output_weight,
    second_gain,
    gate_weight,
    up_weight,
    down_weight,
    grad_out,
):
    rows = hidden_in.shape[0]
    nd, nt = lax.axis_size("dp"), lax.axis_size("tensor")
    dp, tensor = lax.axis_index("dp"), lax.axis_index("tensor")
    full = rows * nt
    width = hidden_in.shape[2]
    small_rows = first_gain.shape[0]

    pack = jnp.concatenate(
        [
            key_basis,
            value_basis,
            key_heads,
            value_heads,
            jnp.zeros((small_rows, KV_COLS - 256 - 2 * KV_HEADS), BF),
            query_basis,
            query_heads,
            first_gain[:, None],
            second_gain[:, None],
            jnp.zeros((small_rows, Q_COLS - Q_BASIS - Q_HEADS - 2), BF),
        ],
        axis=1,
    )
    small_own, small_got = gather_dense(pack, ("z", "x", "y"))
    small_me = (dp * nt + tensor).astype(jnp.int32)[None]
    factor_weight = place_small(small_me, small_own, small_got, nd, nt).reshape(width, PACK)
    gain_at = KV_COLS + Q_BASIS + Q_HEADS
    gains = factor_weight[:, gain_at : gain_at + 2].astype(F32).T
    gain_first, gain_second = gains[0:1], gains[1:2]

    first_pack = jnp.concatenate([output_weight.T, gate_weight], axis=1)
    second_pack = jnp.concatenate([up_weight, down_weight.T], axis=1)
    first_pack, second_pack, factor_weight = lax.optimization_barrier(
        (first_pack, second_pack, factor_weight)
    )
    first_got = gather_dense(first_pack, ("z", "x", "y"))
    second_got = gather_dense(second_pack, ("z", "y", "x"))

    half_dim = DH // 2
    frequency = jnp.exp(jnp.arange(half_dim, dtype=F32) * (-math.log(ROPE_BASE) / half_dim))
    angles = jnp.arange(full, dtype=jnp.int32).astype(F32)[:, None] * frequency[None, :]
    cosine = jnp.tile(jnp.cos(angles), (1, 4))
    sine = jnp.tile(jnp.sin(angles), (1, 4))
    own_cosine = lax.dynamic_slice_in_dim(cosine, tensor * rows, rows, 0)
    own_sine = lax.dynamic_slice_in_dim(sine, tensor * rows, rows, 0)
    q_spread = spread_matrix(RQ, 0)
    k_spread = spread_matrix(RKV, 0)
    v_spread = spread_matrix(RKV, KV_HEADS)

    hidden = hidden_in[:, 0, :].astype(F32)
    first_scale = rms_scale(hidden)
    normed = (hidden * first_scale * gain_first).astype(BF)
    factors = dot(normed, factor_weight).astype(BF)
    kv_factors = gather_stage(factors[:, :KV_COLS], "y")
    q_factors = factors[:, KV_COLS:]
    tensor_me = tensor.astype(jnp.int32)[None]
    queries = build_queries(q_factors, own_cosine, own_sine, q_spread)
    keys, values = build_keys(tensor_me, kv_factors, cosine, sine, k_spread, v_spread)

    where = jnp.stack([tensor * rows, prefix_len[0]]).astype(jnp.int32)
    attended, log_total = attention(where, queries, keys, values)

    out_t, gate, up, down_t = place_weights(
        jnp.stack([dp, tensor]).astype(jnp.int32),
        first_got,
        second_got,
        (output_weight.shape[0], gate_weight.shape[1], up_weight.shape[1], down_weight.shape[0]),
        nd,
        nt,
    )

    middle = hidden + dot(attended, out_t, NT)
    second_scale = rms_scale(middle)
    normed_second = (middle * second_scale * gain_second).astype(BF)
    gate_pre = dot(normed_second, gate)
    upward = dot(normed_second, up)
    gate_sigmoid = jax.nn.sigmoid(gate_pre)
    activated = (gate_pre * gate_sigmoid * upward).astype(BF)
    hidden_out = (middle + dot(activated, down_t, NT)).astype(BF)

    g = grad_out[:, 0, :]
    grad_active = dot(g, down_t)
    grad_gate = (
        grad_active * upward * gate_sigmoid * (1.0 + gate_pre * (1.0 - gate_sigmoid))
    ).astype(BF)
    grad_up = (grad_active * gate_pre * gate_sigmoid).astype(BF)
    hid = gate_weight.shape[1]

    def share(array, t, size):
        return array[:, t * size : (t + 1) * size]

    down_parts = [[dot(g, share(activated, t, hid), TN).astype(BF)] for t in range(nt)]
    gate_parts = [[dot(normed_second, share(grad_gate, t, hid), TN).astype(BF)] for t in range(nt)]
    up_parts = [[dot(normed_second, share(grad_up, t, hid), TN).astype(BF)] for t in range(nt)]
    grad_normed_second = dot(grad_gate, gate, NT) + dot(grad_up, up, NT)
    back_second, second_gain_part = norm_back(middle, second_scale, gain_second, grad_normed_second)
    grad_middle = g.astype(F32) + back_second
    grad_branch = grad_middle.astype(BF)
    out_rows = output_weight.shape[0]
    out_parts = [[dot(grad_branch, share(attended, t, out_rows), TN).astype(BF)] for t in range(nt)]
    grad_heads = dot(grad_branch, out_t).astype(BF)

    down_sum = scatter_sum(down_parts, ("core", "y", "x", "z"))[0]
    gate_sum = scatter_sum(gate_parts, ("core", "x", "y", "z"))[0]
    up_sum, out_sum = scatter_sum(
        [up_parts[t] + out_parts[t] for t in range(nt)], ("core", "y", "x", "z")
    )

    pairs = HEADS // 2
    calls = 4
    query_grads, key_grads, value_grads = [], [], []
    for call in range(calls):
        count = pairs // calls
        dq, dk, dv = attention_back(
            where, queries, keys, values, grad_heads, attended, log_total, call * count, count
        )
        query_grads.append(dq)
        key_grads.append(dk)
        value_grads.append(dv)
    query_grad = jnp.concatenate(query_grads, axis=1)
    key_grad = jnp.concatenate(key_grads, axis=1)
    value_grad = jnp.concatenate(value_grads, axis=1)

    q_factor_grad = queries_back(q_factors, own_cosine, own_sine, q_spread, query_grad)
    kv_parts = keys_back(
        tensor_me, kv_factors, cosine, sine, k_spread, v_spread, key_grad, value_grad
    )
    axis, masks = stage_masks("y")
    kv_total = kv_parts[0].astype(F32)
    for step, mask in enumerate(masks, 1):
        kv_total = kv_total + swap(kv_parts[step], axis, mask).astype(F32)
    factor_grad = jnp.concatenate([kv_total.astype(BF), q_factor_grad], axis=1)

    keep = jnp.arange(PACK) < gain_at
    keep = keep & ~((jnp.arange(PACK) >= 256 + 2 * KV_HEADS) & (jnp.arange(PACK) < KV_COLS))
    factor_grad = jnp.where(keep[None], factor_grad, BF(0))
    grad_normed = dot(factor_grad, factor_weight, NT)
    back_first, first_gain_part = norm_back(hidden, first_scale, gain_first, grad_normed)
    grad_in = grad_middle + back_first
    weight_grad = dot(normed, factor_grad, TN)
    column = jnp.arange(PACK)[None]
    weight_grad = jnp.where(
        column == gain_at,
        first_gain_part[:, None],
        jnp.where(column == gain_at + 1, second_gain_part[:, None], weight_grad),
    ).astype(BF)
    small = weight_grad.reshape(nd, nt, small_rows, PACK)
    small_parts = [[small[:, t].reshape(nd * small_rows, PACK)] for t in range(nt)]
    small_sum = scatter_sum(small_parts, ("core", "y", "x", "z"))[0]

    return (
        hidden_out[:, None, :],
        grad_in[:, None, :],
        small_sum[:, gain_at],
        small_sum[:, KV_COLS + Q_BASIS : gain_at],
        small_sum[:, KV_COLS : KV_COLS + Q_BASIS],
        small_sum[:, 256 : 256 + KV_HEADS],
        small_sum[:, 0:128],
        small_sum[:, 256 + KV_HEADS : 256 + 2 * KV_HEADS],
        small_sum[:, 128:256],
        out_sum.T,
        small_sum[:, gain_at + 1],
        gate_sum,
        up_sum,
        down_sum.T,
    )


def solution(mesh):
    placed = (
        P("tensor", "dp", None),
        P("dp"),
        P(("dp", "tensor")),
        P(("dp", "tensor"), None),
        P(("dp", "tensor"), None),
        P(("dp", "tensor"), None),
        P(("dp", "tensor"), None),
        P(("dp", "tensor"), None),
        P(("dp", "tensor"), None),
        P("tensor", "dp"),
        P(("dp", "tensor")),
        P("dp", "tensor"),
        P("dp", "tensor"),
        P("tensor", "dp"),
        P("tensor", "dp", None),
    )
    return jax.shard_map(
        per_device,
        mesh=mesh,
        in_specs=placed,
        out_specs=(
            P("tensor", "dp", None),
            P("tensor", "dp", None),
            P(("dp", "tensor")),
            P(("dp", "tensor"), None),
            P(("dp", "tensor"), None),
            P(("dp", "tensor"), None),
            P(("dp", "tensor"), None),
            P(("dp", "tensor"), None),
            P(("dp", "tensor"), None),
            P("tensor", "dp"),
            P(("dp", "tensor")),
            P("dp", "tensor"),
            P("dp", "tensor"),
            P("tensor", "dp"),
        ),
        check_vma=False,
    )
```
